32 devices in a mesh: rep: 8 (over y, x, core), tp: 4 (over z).
Axes of the slice: x: 2, y: 2, z: 4, core: 2. Of those that a mesh axis runs over, the one named last changes fastest.
Arguments:
- tokens: bfloat16 [4096, 8192], P('rep'), may hold values from -6 to 6
- query_weight: float32 [8192, 8192], P(('rep', 'tp')), may hold values from -0.0625 to 0.0625
- key_weight: float32 [8192, 1024], P(('rep', 'tp')), may hold values from -0.0625 to 0.0625
- value_weight: float32 [8192, 1024], P(('rep', 'tp')), may hold values from -0.0625 to 0.0625
- cache_keys: bfloat16 [256, 128, 1024], P('rep', None, 'tp'), may hold values from -240 to 240
- cache_values: bfloat16 [256, 128, 1024], P('rep', None, 'tp'), may hold values from -6 to 6
- lengths: int32 [8, 2], P('rep'), may hold values from 1 to 2048
- page_table: int32 [8, 2, 16], P('rep'), may hold values from 0 to 31, as said below
Outputs:
- attended: bfloat16 [4096, 8192], P('rep', 'tp')
- new_cache: bfloat16 [2, 4096, 1024], P(None, 'rep', 'tp')
The draws below stay inside these ranges and needn't reach their ends.
Inputs may be any that keep to these rules, and one draw needn't show every extreme that they name: For each group g, the 2 x 16 entries of page_table[g] name each of the group's local pool pages 0 to 31 exactly once.
All inputs are finite; a program needn't handle non-finite values.
Results may differ from the reference program's by a relative error of at most 0.008.
The reference program's roundings to bfloat16 on the way (of `probs`) count: a program that leaves them out, or rounds other values in their place, can miss the bound.
Values may be sent and summed in bfloat16 or wider, within the bound.
A program may use at most 192 MiB of HBM per device.

```python
import jax
import jax.numpy as jnp
from jax import lax

D = 8192
HEADS = 64
KV_HEADS = 8
HEAD_DIM = 128
SEQS = 2
NEW = 256
PAGE = 128
PAGES_SEQ = 16
REPS = 8
TOK = 512
MAXLEN = 2048
POOL = 32


def draw_cache_keys(key, part):
    shape = (REPS * POOL, PAGE, KV_HEADS * HEAD_DIM)
    base = jnp.clip(jax.random.normal(jax.random.fold_in(key, 11), shape, jnp.float32), -4.0, 4.0)
    return base.astype(jnp.bfloat16)


def draw_page_table(key, part):
    keys = jax.random.split(jax.random.fold_in(key, 21), REPS)
    orders = jax.vmap(lambda single: jax.random.permutation(single, POOL))(keys)
    return orders.astype(jnp.int32).reshape(REPS, SEQS, PAGES_SEQ)


def touch_ends(entries, rng, low, largest):
    spot = [jax.random.randint(jax.random.fold_in(rng, axis), (), 0, length) for axis, length in enumerate(entries.shape)]
    longest = entries.shape.index(max(entries.shape))
    beside = spot[:longest] + [(spot[longest] + 1) % entries.shape[longest]] + spot[longest + 1:]
    return entries.at[tuple(spot)].set(low).at[tuple(beside)].set(largest)


def block_levels(rng, extent, shards, smallest, top_value):
    factor_of, own = 1.0, jax.random.fold_in(rng, 6)
    for axis_at, shards_of in shards:
        steps = jnp.exp(jax.random.uniform(jax.random.fold_in(own, axis_at), (shards_of,), jnp.float32, smallest / len(shards), top_value / len(shards)))
        factor_of = factor_of * jnp.repeat(steps, extent[axis_at] // shards_of).reshape([-1 if axis == axis_at else 1 for axis in range(len(extent))])
    return factor_of


def gaussian(stream_key, dims, deviation, reach, shards=(), held_as=jnp.bfloat16):
    level = block_levels(stream_key, dims, shards, -0.22, 0.18) if shards else 1.0
    values = jax.random.normal(stream_key, dims, jnp.float32) * deviation * level
    return jnp.minimum(jnp.maximum(values, -reach), reach).astype(held_as)


def setup_inputs(seed: int = 0) -> dict:
    splits = jax.random.split(jax.random.key(seed), 9)
    tokens = gaussian(splits[0], (REPS * TOK, D), 1.0, 6.0, ((0, 8),))
    query_weight = gaussian(splits[1], (D, HEADS * HEAD_DIM), D ** -0.5, 0.0625, ((0, 32),), jnp.float32)
    key_weight = gaussian(splits[2], (D, KV_HEADS * HEAD_DIM), D ** -0.5, 0.0625, ((0, 32),), jnp.float32)
    value_weight = gaussian(splits[3], (D, KV_HEADS * HEAD_DIM), D ** -0.5, 0.0625, ((0, 32),), jnp.float32)
    cache_keys = draw_cache_keys(jax.random.fold_in(splits[8], 71), 0)
    cache_values = gaussian(splits[5], (REPS * POOL, PAGE, KV_HEADS * HEAD_DIM), 1.0, 6.0, ((0, 8), (2, 4)))
    lengths = touch_ends(jax.random.randint(splits[6], (REPS, SEQS), 1, MAXLEN + 1), jax.random.fold_in(splits[6], 1), 1, MAXLEN).astype(jnp.int32)
    page_table = draw_page_table(jax.random.fold_in(splits[8], 71), 0)
    return dict(tokens=tokens, query_weight=query_weight, key_weight=key_weight, value_weight=value_weight, cache_keys=cache_keys, cache_values=cache_values, lengths=lengths, page_table=page_table)


ROPE_THETA = 500000.0


def rotate(vectors, positions):
    half_dim = HEAD_DIM // 2
    frequency = ROPE_THETA ** (-2.0 * jnp.arange(half_dim, dtype=jnp.float32) / HEAD_DIM)
    angles = positions.astype(jnp.float32)[:, None] * frequency[None, :]
    cosine_part = jnp.cos(angles)[:, None, :]
    sine_part = jnp.sin(angles)[:, None, :]
    first_half = vectors[..., :half_dim]
    second_half = vectors[..., half_dim:]
    return jnp.concatenate([first_half * cosine_part - second_half * sine_part, second_half * cosine_part + first_half * sine_part], axis=-1)


def reference(tokens, query_weight, key_weight, value_weight, cache_keys, cache_values, lengths, page_table):
    query_bf = query_weight.astype(jnp.bfloat16)
    key_bf = key_weight.astype(jnp.bfloat16)
    value_bf = value_weight.astype(jnp.bfloat16)
    group_size = HEADS // KV_HEADS
    scale = 1.0 / (HEAD_DIM ** 0.5)
    key_pool = cache_keys.reshape(REPS, POOL, PAGE, KV_HEADS * HEAD_DIM)
    value_pool = cache_values.reshape(REPS, POOL, PAGE, KV_HEADS * HEAD_DIM)

    def one_group(items):
        group_tokens, pool_keys, pool_values, group_lengths, group_pages = items
        raw_query = jnp.dot(group_tokens, query_bf, preferred_element_type=jnp.float32)
        raw_key = jnp.dot(group_tokens, key_bf, preferred_element_type=jnp.float32)
        raw_value = jnp.dot(group_tokens, value_bf, preferred_element_type=jnp.float32)
        positions = (group_lengths[:, None] + jnp.arange(NEW, dtype=jnp.int32)[None, :]).reshape(TOK)
        queries = rotate(raw_query.reshape(TOK, HEADS, HEAD_DIM), positions).astype(jnp.bfloat16)
        new_keys = rotate(raw_key.reshape(TOK, KV_HEADS, HEAD_DIM), positions).astype(jnp.bfloat16)
        new_values = raw_value.astype(jnp.bfloat16).reshape(TOK, KV_HEADS, HEAD_DIM)

        def one_sequence(inner):
            seq_queries, seq_keys, seq_values, page_rows, length = inner
            old_keys = pool_keys[page_rows].reshape(MAXLEN, KV_HEADS, HEAD_DIM)
            old_values = pool_values[page_rows].reshape(MAXLEN, KV_HEADS, HEAD_DIM)
            all_keys = jnp.concatenate([old_keys, seq_keys], axis=0).astype(jnp.float32)
            all_values = jnp.concatenate([old_values, seq_values], axis=0).astype(jnp.float32)
            grouped = seq_queries.reshape(NEW, KV_HEADS, group_size, HEAD_DIM).astype(jnp.float32)
            scores = jnp.einsum("nkgd,mkd->kgnm", grouped, all_keys) * scale
            key_index = jnp.arange(MAXLEN + NEW, dtype=jnp.int32)[None, :]
            query_index = jnp.arange(NEW, dtype=jnp.int32)[:, None]
            visible = jnp.where(key_index < MAXLEN, key_index < length, key_index - MAXLEN <= query_index)
            scores = jnp.where(visible[None, None], scores, -1e30)
            maxima = jnp.max(scores, axis=-1, keepdims=True)
            expons = jnp.exp(scores - maxima)
            probs = (expons / jnp.sum(expons, axis=-1, keepdims=True)).astype(jnp.bfloat16)
            output = jnp.einsum("kgnm,mkd->nkgd", probs.astype(jnp.float32), all_values)
            return output.astype(jnp.bfloat16).reshape(NEW, HEADS * HEAD_DIM)

        attended = lax.map(one_sequence, (queries.reshape(SEQS, NEW, HEADS, HEAD_DIM), new_keys.reshape(SEQS, NEW, KV_HEADS, HEAD_DIM), new_values.reshape(SEQS, NEW, KV_HEADS, HEAD_DIM), group_pages, group_lengths))
        return attended.reshape(TOK, HEADS * HEAD_DIM), new_keys.reshape(TOK, KV_HEADS * HEAD_DIM), new_values.reshape(TOK, KV_HEADS * HEAD_DIM)

    attended, key_rows, value_rows = lax.map(one_group, (tokens.reshape(REPS, TOK, D), key_pool, value_pool, lengths, page_table))
    new_cache = jnp.stack([key_rows.reshape(REPS * TOK, KV_HEADS * HEAD_DIM), value_rows.reshape(REPS * TOK, KV_HEADS * HEAD_DIM)])
    return attended.reshape(REPS * TOK, HEADS * HEAD_DIM), new_cache
```

```python
import functools
import math

import jax
import jax.numpy as jnp
from jax import lax
from jax.experimental import pallas as pl
from jax.experimental.pallas import tpu as pltpu
from jax.sharding import PartitionSpec as P

HEADS = 64
KV_HEADS = 8
HEAD_DIM = 128
CHUNK_HEADS = 4
ROPE_THETA = 500000.0


def rope_tables(positions):
    half_dim = HEAD_DIM // 2
    frequency = ROPE_THETA ** (-2.0 * jnp.arange(half_dim, dtype=jnp.float32) / HEAD_DIM)
    angles = positions.astype(jnp.float32)[:, None] * frequency[None, :]
    cosine = jnp.cos(angles)
    sine = jnp.sin(angles)
    return (
        jnp.concatenate([cosine, cosine], axis=-1),
        jnp.concatenate([-sine, sine], axis=-1),
    )


def rotate(vectors, cosine, sine):
    half_dim = HEAD_DIM // 2
    swapped = jnp.concatenate([vectors[..., half_dim:], vectors[..., :half_dim]], axis=-1)
    return vectors * cosine[:, None, :] + swapped * sine[:, None, :]


def attention_kernel(*refs):
    raw_ref, cos_ref, sin_ref, old_k, old_v, new_k, new_v, bias_ref = refs[:8]
    out_ref = refs[-1]
    factor = math.log2(math.e) / math.sqrt(HEAD_DIM)
    raw = raw_ref[...]
    query = raw * cos_ref[...] + pltpu.roll(raw, HEAD_DIM // 2, 1) * sin_ref[...]
    query = query.astype(jnp.bfloat16)
    contract = (((1,), (1,)), ((), ()))
    far = lax.dot_general(query, old_k[0], contract, preferred_element_type=jnp.float32)
    far = far + bias_ref[0]
    near = lax.dot_general(query, new_k[...], contract, preferred_element_type=jnp.float32)
    row = lax.broadcasted_iota(jnp.int32, near.shape, 0)
    column = lax.broadcasted_iota(jnp.int32, near.shape, 1)
    near = jnp.where(column <= row, near, -1e30)
    top = jnp.maximum(
        jnp.max(far, axis=-1, keepdims=True), jnp.max(near, axis=-1, keepdims=True)
    )
    far = jnp.exp2((far - top) * factor)
    near = jnp.exp2((near - top) * factor)
    total = jnp.sum(far, axis=-1, keepdims=True) + jnp.sum(near, axis=-1, keepdims=True)
    result = jnp.dot(far.astype(jnp.bfloat16), old_v[0], preferred_element_type=jnp.float32)
    result += jnp.dot(near.astype(jnp.bfloat16), new_v[...], preferred_element_type=jnp.float32)
    out_ref[...] = (result / total).astype(jnp.bfloat16)


def attention(chunk, raw, cosine, sine, old_k, old_v, new_cache_k, new_cache_v, bias, held, width):
    seqs, cached, _ = old_k.shape
    tok = raw.shape[0]
    new = tok // seqs
    heads = raw.shape[1] // HEAD_DIM
    kv = chunk * CHUNK_HEADS // (HEADS // KV_HEADS)
    in_specs = [
        pl.BlockSpec((new, HEAD_DIM), lambda s, h: (s, h)),
        pl.BlockSpec((new, HEAD_DIM), lambda s, h: (s, 0)),
        pl.BlockSpec((new, HEAD_DIM), lambda s, h: (s, 0)),
        pl.BlockSpec((1, cached, HEAD_DIM), lambda s, h: (s, 0, kv)),
        pl.BlockSpec((1, cached, HEAD_DIM), lambda s, h: (s, 0, kv)),
        pl.BlockSpec((new, HEAD_DIM), lambda s, h: (s, kv)),
        pl.BlockSpec((new, HEAD_DIM), lambda s, h: (s, kv)),
        pl.BlockSpec((1, 1, cached), lambda s, h: (s, 0, 0)),
    ]
    operands = [raw, cosine, sine, old_k, old_v, new_cache_k, new_cache_v, bias]
    aliases = {}
    if held is not None:
        in_specs.append(pl.BlockSpec(memory_space=pl.ANY))
        operands.append(held)
        aliases = {8: 0}
    keys = cached + new
    return pl.pallas_call(
        attention_kernel,
        grid=(seqs, heads),
        out_shape=jax.ShapeDtypeStruct((tok, width), jnp.bfloat16),
        in_specs=in_specs,
        out_specs=pl.BlockSpec((new, HEAD_DIM), lambda s, h: (s, chunk * CHUNK_HEADS + h)),
        input_output_aliases=aliases,
        compiler_params=pltpu.CompilerParams(vmem_limit_bytes=32 * 1024 * 1024),
        cost_estimate=pl.CostEstimate(
            flops=4 * tok * heads * keys * HEAD_DIM,
            bytes_accessed=2 * 2 * seqs * keys * HEAD_DIM + 6 * tok * heads * HEAD_DIM,
            transcendentals=tok * heads * keys,
        ),
    )(*operands)


def per_device(
    tp,
    tokens,
    query_weight,
    key_weight,
    value_weight,
    cache_keys,
    cache_values,
    lengths,
    page_table,
):
    kv_local = KV_HEADS // tp
    kv_width = kv_local * HEAD_DIM
    q_width = HEADS // tp * HEAD_DIM
    chunk_width = CHUNK_HEADS * HEAD_DIM
    tok = tokens.shape[0]
    seqs, pages = page_table.shape[1:]
    new = tok // seqs
    page = cache_keys.shape[1]

    def slab(parts):
        local = jnp.stack(parts).astype(jnp.bfloat16)
        mixed = lax.all_to_all(local, "tp", split_axis=0, concat_axis=0, tiled=True)
        rows = mixed.reshape(-1, mixed.shape[-1])
        return lax.all_gather(rows, "rep", axis=0, tiled=True)

    def columns(weight, start, width, whole):
        return [weight[:, t * whole + start : t * whole + start + width] for t in range(tp)]

    slabs = [
        slab(
            [
                jnp.concatenate(pair, axis=1)
                for pair in zip(
                    columns(key_weight, 0, kv_width, kv_width),
                    columns(value_weight, 0, kv_width, kv_width),
                )
            ]
        )
    ]
    for start in range(0, q_width, chunk_width):
        slabs.append(slab(columns(query_weight, start, chunk_width, q_width)))

    seq_lengths = lengths[0]
    positions = (seq_lengths[:, None] + jnp.arange(new, dtype=jnp.int32)[None, :]).reshape(tok)
    cosine, sine = rope_tables(positions)
    order = page_table[0].reshape(-1)
    old_k = cache_keys[order].reshape(seqs, pages * page, kv_width)
    old_v = cache_values[order].reshape(seqs, pages * page, kv_width)
    visible = jnp.arange(pages * page, dtype=jnp.int32)[None, :] < seq_lengths[:, None]
    bias = jnp.where(visible, 0.0, -1e30).astype(jnp.float32)[:, None, :]

    raw_kv = jnp.dot(tokens, slabs[0], preferred_element_type=jnp.float32)
    new_k = rotate(raw_kv[:, :kv_width].reshape(tok, kv_local, HEAD_DIM), cosine, sine)
    new_k = new_k.astype(jnp.bfloat16).reshape(tok, kv_width)
    new_v = raw_kv[:, kv_width:].astype(jnp.bfloat16)

    attended = None
    for chunk, piece in enumerate(slabs[1:]):
        raw = jnp.dot(tokens, piece, preferred_element_type=jnp.float32)
        attended = attention(
            chunk, raw, cosine, sine, old_k, old_v, new_k, new_v, bias, attended, q_width
        )
    return attended, jnp.stack([new_k, new_v])


def solution(mesh):
    return jax.shard_map(
        functools.partial(per_device, mesh.shape["tp"]),
        mesh=mesh,
        in_specs=(
            P("rep", None),
            P(("rep", "tp"), None),
            P(("rep", "tp"), None),
            P(("rep", "tp"), None),
            P("rep", None, "tp"),
            P("rep", None, "tp"),
            P("rep", None),
            P("rep", None, None),
        ),
        out_specs=(P("rep", "tp"), P(None, "rep", "tp")),
        check_vma=False,
    )
```
